16 devices in a mesh: dp: 4 (over z, y), tp: 4 (over x, core).
Axes of the slice: x: 2, y: 2, z: 2, core: 2. Of those that a mesh axis runs over, the one named last changes fastest.
Arguments:
- x: bfloat16 [16, 1024, 1152], P('dp', 'tp'), parts along dimension 0
- d_out: bfloat16 [16, 1024, 1152], P('dp', 'tp'), parts along dimension 0
- ln1_gain: float32 [1152], replicated
- ln1_bias: float32 [1152], replicated
- w_q: bfloat16 [1152, 16, 72], P(None, 'tp')
- b_q: bfloat16 [16, 72], P('tp')
- w_k: bfloat16 [1152, 16, 72], P(None, 'tp')
- w_v: bfloat16 [1152, 16, 72], P(None, 'tp')
- b_v: bfloat16 [16, 72], P('tp')
- w_o: bfloat16 [16, 72, 1152], P('tp')
- b_o: bfloat16 [1152], replicated
- ln2_gain: float32 [1152], replicated
- ln2_bias: float32 [1152], replicated
- w_1: bfloat16 [1152, 4304], P(None, 'tp')
- b_1: bfloat16 [4304], P('tp')
- w_2: bfloat16 [4304, 1152], P('tp')
- b_2: bfloat16 [1152], replicated
Outputs:
- output 1: bfloat16 [16, 1024, 1152], P('dp', 'tp'), parts along dimension 0
- output 2: bfloat16 [16, 1024, 1152], P('dp', 'tp'), parts along dimension 0
- output 3: float32 [4608], P('dp'), parts along dimension 0
- output 4: float32 [4608], P('dp'), parts along dimension 0
- output 5: bfloat16 [4608, 16, 72], P('dp', 'tp'), parts along dimension 0
- output 6: bfloat16 [64, 72], P(('dp', 'tp')), parts along dimension 0
- output 7: bfloat16 [4608, 16, 72], P('dp', 'tp'), parts along dimension 0
- output 8: bfloat16 [4608, 16, 72], P('dp', 'tp'), parts along dimension 0
- output 9: bfloat16 [64, 72], P(('dp', 'tp')), parts along dimension 0
- output 10: bfloat16 [64, 72, 1152], P(('dp', 'tp')), parts along dimension 0
- output 11: bfloat16 [4608], P('dp'), parts along dimension 0
- output 12: float32 [4608], P('dp'), parts along dimension 0
- output 13: float32 [4608], P('dp'), parts along dimension 0
- output 14: bfloat16 [4608, 4304], P('dp', 'tp'), parts along dimension 0
- output 15: bfloat16 [17216], P(('dp', 'tp')), parts along dimension 0
- output 16: bfloat16 [17216, 1152], P(('dp', 'tp')), parts along dimension 0
- output 17: bfloat16 [4608], P('dp'), parts along dimension 0
There are 4 independent parts. The reference program is written for one: setup_inputs(seed, part) draws one part's arguments, and reference() takes and returns one part's arrays. A program takes and returns all parts, laid end to end along the dimension named above; an argument that names none is the same for every part.
All inputs are finite; a program needn't handle non-finite values.
Results may differ from the reference program's by a relative error of at most 0.0181033.
Values are sent between devices in bfloat16 or wider.
A program may use at most 1 GiB of HBM per device.

```python
import math
import jax
import jax.numpy as jnp
from jax import lax

IMAGES = 4
PATCHES = 1024
WIDTH = 1152
NUM_HEADS = 16
HEAD_DIM = 72
MLP_DIM = 4304
LN_EPS = 1e-6
ATT_SCALE = 1.0 / math.sqrt(HEAD_DIM)
TOKENS = IMAGES * PATCHES


def draw_normal(key, shape, scale):
    return jax.random.normal(key, shape, jnp.float32) * scale


def setup_inputs(seed: int = 0, part: int = 0) -> dict:
    part_key = jax.random.fold_in(jax.random.key(seed), part)
    act_keys = jax.random.split(part_key, 4)
    wt_keys = jax.random.split(jax.random.key(seed + 1), 15)
    act_shape = (IMAGES, PATCHES, WIDTH)
    row_scale = jnp.exp(draw_normal(act_keys[0], (IMAGES, PATCHES, 1), 0.5))
    row_shift = draw_normal(act_keys[1], (IMAGES, PATCHES, 1), 0.5)
    x = (draw_normal(act_keys[2], act_shape, 1.0) * row_scale + row_shift).astype(jnp.bfloat16)
    d_out = draw_normal(act_keys[3], act_shape, 1.0).astype(jnp.bfloat16)
    in_scale = WIDTH ** -0.5
    qk_scale = in_scale * math.sqrt(math.sqrt(math.log(PATCHES / 8.0)))
    head_w = (WIDTH, NUM_HEADS, HEAD_DIM)
    head_b = (NUM_HEADS, HEAD_DIM)
    return {
        'x': x,
        'd_out': d_out,
        'ln1_gain': 1.0 + draw_normal(wt_keys[0], (WIDTH,), 0.25),
        'ln1_bias': draw_normal(wt_keys[1], (WIDTH,), 0.3),
        'w_q': draw_normal(wt_keys[2], head_w, qk_scale).astype(jnp.bfloat16),
        'b_q': draw_normal(wt_keys[3], head_b, 0.5).astype(jnp.bfloat16),
        'w_k': draw_normal(wt_keys[4], head_w, qk_scale).astype(jnp.bfloat16),
        'w_v': draw_normal(wt_keys[5], head_w, in_scale).astype(jnp.bfloat16),
        'b_v': draw_normal(wt_keys[6], head_b, 0.5).astype(jnp.bfloat16),
        'w_o': draw_normal(wt_keys[7], (NUM_HEADS, HEAD_DIM, WIDTH), 2.5 * in_scale).astype(jnp.bfloat16),
        'b_o': draw_normal(wt_keys[8], (WIDTH,), 0.5).astype(jnp.bfloat16),
        'ln2_gain': 1.0 + draw_normal(wt_keys[9], (WIDTH,), 0.25),
        'ln2_bias': draw_normal(wt_keys[10], (WIDTH,), 0.3),
        'w_1': draw_normal(wt_keys[11], (WIDTH, MLP_DIM), in_scale).astype(jnp.bfloat16),
        'b_1': draw_normal(wt_keys[12], (MLP_DIM,), 0.5).astype(jnp.bfloat16),
        'w_2': draw_normal(wt_keys[13], (MLP_DIM, WIDTH), 1.5 * MLP_DIM ** -0.5).astype(jnp.bfloat16),
        'b_2': draw_normal(wt_keys[14], (WIDTH,), 0.5).astype(jnp.bfloat16),
    }


def layer_norm(rows, ln_gain, ln_bias):
    row_mean = jnp.mean(rows, axis=-1, keepdims=True)
    centered = rows - row_mean
    variance = jnp.mean(centered * centered, axis=-1, keepdims=True)
    return centered * lax.rsqrt(variance + LN_EPS) * ln_gain + ln_bias


def attend_image(qkv_image):
    queries, keys, values = qkv_image
    scores = jnp.einsum('qhd,khd->hqk', queries.astype(jnp.float32), keys.astype(jnp.float32)) * ATT_SCALE
    probs = jax.nn.softmax(scores, axis=-1).astype(jnp.bfloat16)
    mixed = jnp.einsum('hqk,khd->qhd', probs.astype(jnp.float32), values.astype(jnp.float32))
    return mixed.astype(jnp.bfloat16)


def forward(x, ln1_gain, ln1_bias, w_q, b_q, w_k, w_v, b_v, w_o, b_o, ln2_gain, ln2_bias, w_1, b_1, w_2, b_2):
    x_f32 = x.reshape(TOKENS, WIDTH).astype(jnp.float32)
    h_one = layer_norm(x_f32, ln1_gain, ln1_bias).astype(jnp.bfloat16)
    w_qkv = jnp.concatenate([w_q.reshape(WIDTH, WIDTH), w_k.reshape(WIDTH, WIDTH), w_v.reshape(WIDTH, WIDTH)], axis=1)
    b_qkv = jnp.concatenate([b_q.reshape(WIDTH).astype(jnp.float32), jnp.zeros((WIDTH,), jnp.float32), b_v.reshape(WIDTH).astype(jnp.float32)])
    qkv = (jnp.dot(h_one, w_qkv, preferred_element_type=jnp.float32) + b_qkv).astype(jnp.bfloat16)
    head_shape = (IMAGES, PATCHES, NUM_HEADS, HEAD_DIM)
    queries = qkv[:, :WIDTH].reshape(head_shape)
    keys = qkv[:, WIDTH:2 * WIDTH].reshape(head_shape)
    values = qkv[:, 2 * WIDTH:].reshape(head_shape)
    mixed = lax.map(attend_image, (queries, keys, values)).reshape(TOKENS, WIDTH)
    attn_out = jnp.dot(mixed, w_o.reshape(WIDTH, WIDTH), preferred_element_type=jnp.float32)
    x_mid = (x_f32 + attn_out + b_o).astype(jnp.bfloat16)
    mid_f32 = x_mid.astype(jnp.float32)
    h_two = layer_norm(mid_f32, ln2_gain, ln2_bias).astype(jnp.bfloat16)
    pre_act = (jnp.dot(h_two, w_1, preferred_element_type=jnp.float32) + b_1).astype(jnp.bfloat16)
    hidden = jax.nn.gelu(pre_act.astype(jnp.float32), approximate=True).astype(jnp.bfloat16)
    mlp_out = jnp.dot(hidden, w_2, preferred_element_type=jnp.float32)
    y_out = (mid_f32 + mlp_out + b_2).astype(jnp.bfloat16)
    return y_out.reshape(IMAGES, PATCHES, WIDTH)


def reference(x, d_out, ln1_gain, ln1_bias, w_q, b_q, w_k, w_v, b_v, w_o, b_o, ln2_gain, ln2_bias, w_1, b_1, w_2, b_2):
    y_out, pullback = jax.vjp(forward, x, ln1_gain, ln1_bias, w_q, b_q, w_k, w_v, b_v, w_o, b_o, ln2_gain, ln2_bias, w_1, b_1, w_2, b_2)
    (grad_x, grad_ln1_gain, grad_ln1_bias, grad_w_q, grad_b_q, grad_w_k, grad_w_v, grad_b_v, grad_w_o, grad_b_o,
     grad_ln2_gain, grad_ln2_bias, grad_w_1, grad_b_1, grad_w_2, grad_b_2) = pullback(d_out)
    return (y_out, grad_x, grad_ln1_gain, grad_ln1_bias, grad_w_q, grad_b_q, grad_w_k, grad_w_v, grad_b_v, grad_w_o, grad_b_o,
            grad_ln2_gain, grad_ln2_bias, grad_w_1, grad_b_1, grad_w_2, grad_b_2)
```

```python
import math
import jax
import jax.numpy as jnp
from jax import lax
from jax.experimental import pallas as pl
from jax.experimental.pallas import tpu as pltpu
from jax.sharding import PartitionSpec as P

LN_EPS = 1e-6
HEAD = 72
PAIR = 2 * HEAD
QBLK = 256
F32 = jnp.float32
BF16 = jnp.bfloat16
LOG2E = 1.4426950408889634


def layer_norm(rows, ln_gain, ln_bias):
    row_mean = jnp.mean(rows, axis=-1, keepdims=True)
    centered = rows - row_mean
    variance = jnp.mean(centered * centered, axis=-1, keepdims=True)
    return centered * lax.rsqrt(variance + LN_EPS) * ln_gain + ln_bias


def gelu_tanh(pre_act):
    return jax.nn.gelu(pre_act, approximate=True)


def dot(a, b):
    return jnp.dot(a, b, preferred_element_type=F32)


def dot_nt(a, b):
    return lax.dot_general(a, b, (((1,), (1,)), ((), ())), preferred_element_type=F32)


def dot_tn(a, b):
    return lax.dot_general(a, b, (((0,), (0,)), ((), ())), preferred_element_type=F32)


def attn_fwd_kernel(q_ref, k_ref, v_ref, o_ref, l_ref):
    tokens = q_ref.shape[1]
    coef = LOG2E / math.sqrt(HEAD)
    q_all = q_ref[...].astype(F32)
    k_all = k_ref[...].astype(F32)
    v_all = v_ref[...].astype(F32)
    keys = [k_all[h * HEAD:(h + 1) * HEAD].T.astype(BF16) for h in range(2)]
    vals = [v_all[h * HEAD:(h + 1) * HEAD].astype(BF16) for h in range(2)]
    quer = [q_all[h * HEAD:(h + 1) * HEAD].astype(BF16) for h in range(2)]
    for start in range(0, tokens, QBLK):
        outs = []
        for h in range(2):
            s = dot(keys[h], quer[h][:, start:start + QBLK])
            top = jnp.max(s, axis=0, keepdims=True)
            e = jnp.exp2((s - top) * coef)
            total = jnp.sum(e, axis=0, keepdims=True)
            p = (e * (1.0 / total)).astype(BF16)
            outs.append(dot(vals[h], p))
            l_ref[0, h:h + 1, start:start + QBLK] = top * coef + jnp.log2(total)
        o_ref[:, start:start + QBLK] = jnp.concatenate(outs, axis=0).astype(BF16)


def attn_bwd_kernel(q_ref, k_ref, v_ref, g_ref, l_ref, d_ref, dk_acc, dv_acc):
    tokens = q_ref.shape[1]
    scale = 1.0 / math.sqrt(HEAD)
    coef = LOG2E * scale
    q_all = q_ref[...].astype(F32)
    k_all = k_ref[...].astype(F32)
    v_all = v_ref[...].astype(F32)
    g_all = g_ref[...].astype(F32)

    def head(a, h):
        return a[h * HEAD:(h + 1) * HEAD]

    k_t = [head(k_all, h).astype(BF16) for h in range(2)]
    keys = [head(k_all, h).T.astype(BF16) for h in range(2)]
    vals = [head(v_all, h).T.astype(BF16) for h in range(2)]
    q_t = [head(q_all, h).astype(BF16) for h in range(2)]
    q_n = [head(q_all, h).T.astype(BF16) for h in range(2)]
    g_t = [head(g_all, h).astype(BF16) for h in range(2)]
    g_n = [head(g_all, h).T.astype(BF16) for h in range(2)]
    for start in range(0, tokens, QBLK):
        cols = slice(start, start + QBLK)
        dqs = []
        for h in range(2):
            s = dot(keys[h], q_t[h][:, cols])
            p = jnp.exp2(s * coef - l_ref[0, h:h + 1, cols])
            dp = dot(vals[h], g_t[h][:, cols]).astype(BF16).astype(F32)
            delta = jnp.sum(p * dp, axis=0, keepdims=True)
            ds = (p * ((dp - delta) * scale)).astype(BF16)
            dv = dot(p.astype(BF16), g_n[h][cols])
            dk = dot(ds, q_n[h][cols])
            if start == 0:
                dv_acc[h] = dv
                dk_acc[h] = dk
            else:
                dv_acc[h] += dv
                dk_acc[h] += dk
            dqs.append(dot(k_t[h], ds))
        d_ref[0, :, cols] = jnp.concatenate(dqs, axis=0).astype(BF16)
    d_ref[1] = jnp.concatenate([dk_acc[h].T for h in range(2)], axis=0).astype(BF16)
    d_ref[2] = jnp.concatenate([dv_acc[h].T for h in range(2)], axis=0).astype(BF16)


def attn_fwd(qkv):
    rows, tokens = qkv.shape
    heads_rows = rows // 3
    pairs = heads_rows // PAIR
    spec = lambda off: pl.BlockSpec((PAIR, tokens), lambda i: (off * pairs + i, 0))
    flops = 4 * heads_rows * tokens * tokens
    return pl.pallas_call(
        attn_fwd_kernel,
        grid=(pairs,),
        in_specs=[spec(0), spec(1), spec(2)],
        out_specs=[spec(0), pl.BlockSpec((1, 8, tokens), lambda i: (i, 0, 0))],
        out_shape=[jax.ShapeDtypeStruct((heads_rows, tokens), BF16), jax.ShapeDtypeStruct((pairs, 8, tokens), F32)],
        cost_estimate=pl.CostEstimate(flops=flops * 4, bytes_accessed=8 * heads_rows * tokens, transcendentals=0),
        name="attn_fwd",
    )(qkv, qkv, qkv)


def attn_bwd(qkv, d_mixed, lse):
    rows, tokens = qkv.shape
    heads_rows = rows // 3
    pairs = heads_rows // PAIR
    spec = lambda off: pl.BlockSpec((PAIR, tokens), lambda i: (off * pairs + i, 0))
    flops = 10 * heads_rows * tokens * tokens
    grads = pl.pallas_call(
        attn_bwd_kernel,
        grid=(pairs,),
        in_specs=[spec(0), spec(1), spec(2), spec(0), pl.BlockSpec((1, 8, tokens), lambda i: (i, 0, 0))],
        out_specs=pl.BlockSpec((3, PAIR, tokens), lambda i: (0, i, 0)),
        out_shape=jax.ShapeDtypeStruct((3, heads_rows, tokens), BF16),
        scratch_shapes=[pltpu.VMEM((2, tokens, HEAD), F32), pltpu.VMEM((2, tokens, HEAD), F32)],
        cost_estimate=pl.CostEstimate(flops=flops * 4, bytes_accessed=16 * heads_rows * tokens, transcendentals=0),
        name="attn_bwd",
    )(qkv, qkv, qkv, d_mixed, lse)
    return grads.reshape(rows, tokens)


def solution(mesh):
    act_spec = P('dp', 'tp', None)
    replicated = P()
    head_w = P(None, 'tp', None)
    head_b = P('tp', None)
    grad_head_w = P('dp', 'tp', None)
    grad_head_b = P(('dp', 'tp'), None)
    grad_vec = P('dp')
    in_specs = (act_spec, act_spec, replicated, replicated, head_w, head_b, head_w, head_w, head_b,
                P('tp', None, None), replicated, replicated, replicated, P(None, 'tp'), P('tp'), P('tp', None), replicated)
    out_specs = (act_spec, act_spec, grad_vec, grad_vec, grad_head_w, grad_head_b, grad_head_w, grad_head_w, grad_head_b,
                 P(('dp', 'tp'), None, None), grad_vec, grad_vec, grad_vec, P('dp', 'tp'), P(('dp', 'tp')),
                 P(('dp', 'tp'), None), grad_vec)

    def swap(value, k):
        return lax.ppermute(value, 'tp', [(i, i ^ k) for i in range(4)])

    def send(block):
        return block, swap(block, 1), swap(block, 2)

    def land(sent, dep):
        own, near, two = sent
        two, _ = lax.optimization_barrier((two, dep))
        return [own, near, two, swap(two, 1)]

    def layer_step(x, d_out, ln1_gain, ln1_bias, w_q, b_q, w_k, w_v, b_v, w_o, b_o, ln2_gain, ln2_bias, w_1, b_1, w_2, b_2):
        me = lax.axis_index('tp')
        width = x.shape[2]
        slab = x.shape[1]
        local_rows = w_o.shape[0] * w_o.shape[1]

        def image(shard, k):
            return lax.dynamic_index_in_dim(shard, me ^ k, 0, keepdims=False)

        def to_image(shard):
            return jnp.concatenate([image(shard, 0)] + [swap(image(shard, k), k) for k in (1, 2, 3)], axis=0)

        def to_tokens(rows):
            parts = [rows[:slab]] + [swap(rows[k * slab:(k + 1) * slab], k) for k in (1, 2, 3)]
            stacked = jnp.stack(parts)
            return jnp.stack([lax.dynamic_index_in_dim(stacked, me ^ i, 0, keepdims=False) for i in range(4)])

        x_img = to_image(x)
        w_qkv_own = jnp.concatenate([w.reshape(width, local_rows).T for w in (w_q, w_k, w_v)], axis=0)
        w_qkv_sent = send(w_qkv_own)
        w_out_sent = send(w_o.reshape(local_rows, width))
        bias_own = jnp.concatenate([b_q.reshape(-1).astype(F32), b_v.reshape(-1).astype(F32), b_1.astype(F32)])
        biases = send(bias_own)
        biases = list(biases) + [swap(biases[2], 1)]
        b_qkv = [jnp.concatenate([b[:local_rows].astype(F32), jnp.zeros((local_rows,), F32),
                                  b[local_rows:2 * local_rows].astype(F32)])[:, None] for b in biases]
        b_one = [b[2 * local_rows:] for b in biases]
        w_one_sent = send(w_1)
        core, chip = lax.rem(me, 2), lax.div(me, 2)
        d_here = lax.dynamic_slice_in_dim(d_out, 2 * chip, 2, 0)
        d_there = lax.dynamic_slice_in_dim(d_out, 2 - 2 * chip, 2, 0)
        d_here_near, d_here_two = swap(d_here, 1), swap(d_there, 2)
        w_two_sent = send(w_2)
        d_there_near, d_there_two = swap(d_there, 1), swap(d_here, 2)

        def rows_of(pairs, which):
            return jnp.concatenate([lax.dynamic_index_in_dim(p, which, 0, keepdims=False) for p in pairs], axis=0)

        x_f32 = x_img.astype(F32)
        h_one_f, ln1_pull = jax.vjp(layer_norm, x_f32, ln1_gain, ln1_bias)
        h_one = h_one_f.astype(BF16)
        qkv, mixed, lse = [], [], []
        w_qkv = list(w_qkv_sent[:2])
        for k in range(4):
            if k == 2:
                w_qkv = land(w_qkv_sent, mixed[1])
            block = (dot_nt(w_qkv[k], h_one) + b_qkv[k]).astype(BF16)
            out, stat = attn_fwd(block)
            qkv.append(block)
            mixed.append(out)
            lse.append(stat)
        w_out = land(w_out_sent, mixed[2])
        attn_out = dot_tn(jnp.concatenate(mixed, axis=0), jnp.concatenate(w_out, axis=0))
        x_mid = (x_f32 + attn_out + b_o).astype(BF16)
        mid_f32 = x_mid.astype(F32)
        h_two_f, ln2_pull = jax.vjp(layer_norm, mid_f32, ln2_gain, ln2_bias)
        h_two = h_two_f.astype(BF16)
        h_sent = send(h_two)

        pre, hid = [], []
        w_one = list(w_one_sent[:2])
        for k in range(4):
            if k == 2:
                w_one = land(w_one_sent, hid[1])
            u = (dot(h_two, w_one[k]) + b_one[k]).astype(BF16)
            pre.append(u)
            hid.append(gelu_tanh(u.astype(F32)).astype(BF16))

        def pull_gelu(u, d_g):
            _, pull = jax.vjp(gelu_tanh, u.astype(F32))
            return pull(d_g.astype(F32))[0].astype(BF16)

        def own_columns(h_rows, d_rows):
            u = (dot(h_rows, w_1) + b_1).astype(BF16)
            g = gelu_tanh(u.astype(F32)).astype(BF16)
            d_u = pull_gelu(u, dot_nt(d_rows, w_2).astype(BF16))
            return h_rows, d_rows, g, d_u

        d_here_two, _ = lax.optimization_barrier((d_here_two, hid[3]))
        d_here_diag = swap(d_here_two, 1)
        d_img = rows_of((d_here, d_here_near, d_here_two, d_here_diag), core)
        d_sib = rows_of((d_here_near, d_here, d_here_diag, d_here_two), 1 - core)
        w_two = list(w_two_sent[:2])
        d_pre = [pull_gelu(pre[k], dot_nt(d_img, w_two[k]).astype(BF16)) for k in range(2)]
        part_sib = own_columns(h_sent[1], d_sib)
        w_two = land(w_two_sent, (part_sib[3], d_pre[1]))
        d_pre += [pull_gelu(pre[k], dot_nt(d_img, w_two[k]).astype(BF16)) for k in (2, 3)]
        mlp_out = dot(hid[0], w_two[0])
        for k in range(1, 4):
            mlp_out += dot(hid[k], w_two[k])
        y_img = (mid_f32 + mlp_out + b_2).astype(BF16)
        y_out = to_tokens(y_img)

        d_h_two_f = dot_nt(d_pre[0], w_one[0])
        for k in range(1, 4):
            d_h_two_f += dot_nt(d_pre[k], w_one[k])
        d_h_two = d_h_two_f.astype(BF16)
        d_mid_ln, g_ln2_gain, g_ln2_bias = ln2_pull(d_h_two.astype(F32))
        d_mid = (d_img.astype(F32) + d_mid_ln).astype(BF16)

        def reduce_cross(part):
            return swap(part[2] + swap(part[3], 1), 2)

        def reduce_near(part, crossed):
            return part[0] + swap(part[1], 1) + crossed

        g_o_part = [dot(mixed[k], d_mid) for k in range(4)]
        g_w_o = reduce_near(g_o_part, reduce_cross(g_o_part))
        d_qkv, g_qkv_part = [None] * 4, [None] * 4
        for k in (3, 2, 1, 0):
            d_mixed = dot_nt(w_out[k], d_mid).astype(BF16)
            d_qkv[k] = attn_bwd(qkv[k], d_mixed, lse[k])
            g_qkv_part[k] = dot(d_qkv[k], h_one)
        g_w_qkv = reduce_near(g_qkv_part, reduce_cross(g_qkv_part)).astype(BF16)
        g_w_q, g_w_k, g_w_v = [g_w_qkv[i * local_rows:(i + 1) * local_rows].T.reshape(w_q.shape) for i in range(3)]

        d_h_one = dot_tn(jnp.concatenate(d_qkv, axis=0), jnp.concatenate(w_qkv, axis=0)).astype(BF16)
        h_all = land(h_sent, d_h_one)
        d_there_two, _ = lax.optimization_barrier((d_there_two, d_mid))
        d_there_diag = swap(d_there_two, 1)
        d_far = jnp.concatenate([rows_of((d_there_two, d_there_diag, d_there, d_there_near), core),
                                 rows_of((d_there_diag, d_there_two, d_there_near, d_there), 1 - core)], axis=0)
        parts = [(h_two, d_img, hid[0], d_pre[0]), part_sib, own_columns(jnp.concatenate(h_all[2:], axis=0), d_far)]
        g_w_1 = sum(dot_tn(h_rows, d_u) for h_rows, _, _, d_u in parts).astype(BF16)
        g_w_2 = sum(dot_tn(g, d_rows) for _, d_rows, g, _ in parts).astype(BF16)
        g_b_1 = sum(jnp.sum(d_u, axis=0, dtype=F32) for _, _, _, d_u in parts).astype(BF16)
        d_in_ln, g_ln1_gain, g_ln1_bias = ln1_pull(d_h_one.astype(F32))
        grad_x_img = (d_mid.astype(F32) + d_in_ln).astype(BF16)
        grad_x = to_tokens(grad_x_img)

        b_part = [jnp.sum(d, axis=1, dtype=F32) for d in d_qkv]
        g_b_qkv = reduce_near(b_part, reduce_cross(b_part)).astype(BF16)
        vecs = jnp.stack([g_ln1_gain, g_ln1_bias, jnp.sum(d_mid, axis=0, dtype=F32), g_ln2_gain, g_ln2_bias,
                          jnp.sum(d_img, axis=0, dtype=F32)])
        vecs = vecs + swap(vecs, 1)
        vecs = vecs + swap(vecs, 2)
        return (y_out, grad_x, vecs[0], vecs[1], g_w_q, g_b_qkv[:local_rows].reshape(b_q.shape), g_w_k, g_w_v,
                g_b_qkv[2 * local_rows:].reshape(b_v.shape), g_w_o.astype(BF16).reshape(w_o.shape),
                vecs[2].astype(BF16), vecs[3], vecs[4], g_w_1, g_b_1, g_w_2, vecs[5].astype(BF16))

    return jax.shard_map(layer_step, mesh=mesh, in_specs=in_specs, out_specs=out_specs, check_vma=False)
```

```python
import math
import jax
import jax.numpy as jnp
from jax import lax
from jax.experimental import pallas as pl
from jax.experimental.pallas import tpu as pltpu
from jax.sharding import PartitionSpec as P

LN_EPS = 1e-6
HEAD = 72
PAIR = 2 * HEAD
FWD_QUERIES = 1024
BWD_QUERIES = 512
ROWS = 512
GELU_C = math.sqrt(2.0 / math.pi)
F32 = jnp.float32
BF16 = jnp.bfloat16
LOG2E = 1.4426950408889634


def layer_norm(rows, ln_gain, ln_bias):
    row_mean = jnp.mean(rows, axis=-1, keepdims=True)
    centered = rows - row_mean
    variance = jnp.mean(centered * centered, axis=-1, keepdims=True)
    return centered * lax.rsqrt(variance + LN_EPS) * ln_gain + ln_bias


def dot(a, b):
    return jnp.dot(a, b, preferred_element_type=F32)


def dot_nt(a, b):
    return lax.dot_general(a, b, (((1,), (1,)), ((), ())), preferred_element_type=F32)


def dot_tn(a, b):
    return lax.dot_general(a, b, (((0,), (0,)), ((), ())), preferred_element_type=F32)


def attn_fwd_kernel(w_ref, b_ref, h_ref, qkv_ref, o_ref, l_ref):
    tokens = h_ref.shape[1]
    coef = LOG2E / math.sqrt(HEAD)
    parts = [(dot(w_ref[i], h_ref[...]) + b_ref[i]).astype(BF16) for i in range(3)]
    for i in range(3):
        qkv_ref[i] = parts[i]
    q_all, k_all, v_all = [part.astype(F32) for part in parts]
    keys = [k_all[h * HEAD:(h + 1) * HEAD].T.astype(BF16) for h in range(2)]
    vals = [v_all[h * HEAD:(h + 1) * HEAD].astype(BF16) for h in range(2)]
    quer = [q_all[h * HEAD:(h + 1) * HEAD].astype(BF16) for h in range(2)]
    for start in range(0, tokens, FWD_QUERIES):
        outs = []
        for h in range(2):
            s = dot(keys[h], quer[h][:, start:start + FWD_QUERIES])
            top = jnp.max(s, axis=0, keepdims=True)
            e = jnp.exp2((s - top) * coef)
            total = jnp.sum(e, axis=0, keepdims=True)
            p = (e * (1.0 / total)).astype(BF16)
            outs.append(dot(vals[h], p))
            l_ref[0, h:h + 1, start:start + FWD_QUERIES] = top * coef + jnp.log2(total)
        o_ref[:, start:start + FWD_QUERIES] = jnp.concatenate(outs, axis=0).astype(BF16)


def attn_bwd_kernel(qkv_ref, g_ref, l_ref, h_ref, d_ref, gw_ref, gb_ref, dk_acc, dv_acc):
    tokens = h_ref.shape[0]
    scale = 1.0 / math.sqrt(HEAD)
    coef = LOG2E * scale
    q_all, k_all, v_all = [qkv_ref[i].astype(F32) for i in range(3)]
    g_all = g_ref[...].astype(F32)

    def head(a, h):
        return a[h * HEAD:(h + 1) * HEAD]

    k_t = [head(k_all, h).astype(BF16) for h in range(2)]
    keys = [head(k_all, h).T.astype(BF16) for h in range(2)]
    vals = [head(v_all, h).T.astype(BF16) for h in range(2)]
    q_t = [head(q_all, h).astype(BF16) for h in range(2)]
    q_n = [head(q_all, h).T.astype(BF16) for h in range(2)]
    g_t = [head(g_all, h).astype(BF16) for h in range(2)]
    g_n = [head(g_all, h).T.astype(BF16) for h in range(2)]
    for start in range(0, tokens, BWD_QUERIES):
        cols = slice(start, start + BWD_QUERIES)
        dqs = []
        for h in range(2):
            s = dot(keys[h], q_t[h][:, cols])
            p = jnp.exp2(s * coef - l_ref[0, h:h + 1, cols])
            dp = dot(vals[h], g_t[h][:, cols]).astype(BF16).astype(F32)
            delta = jnp.sum(p * dp, axis=0, keepdims=True)
            ds = (p * ((dp - delta) * scale)).astype(BF16)
            dv = dot(p.astype(BF16), g_n[h][cols])
            dk = dot(ds, q_n[h][cols])
            if start == 0:
                dv_acc[h] = dv
                dk_acc[h] = dk
            else:
                dv_acc[h] += dv
                dk_acc[h] += dk
            dqs.append(dot(k_t[h], ds))
        d_ref[0, :, cols] = jnp.concatenate(dqs, axis=0).astype(BF16)
    d_ref[1] = jnp.concatenate([dk_acc[h].T for h in range(2)], axis=0).astype(BF16)
    d_ref[2] = jnp.concatenate([dv_acc[h].T for h in range(2)], axis=0).astype(BF16)
    ones = jnp.ones((8, tokens), BF16)
    for i in range(3):
        gw_ref[i] = dot(d_ref[i], h_ref[...])
        gb_ref[i, 0] = dot_nt(ones, d_ref[i])


def attn_fwd(w, bias, h_one):
    _, rows, width = w.shape
    tokens = h_one.shape[1]
    pairs = rows // PAIR
    flops = 16 * rows * tokens * tokens + 6 * rows * tokens * width
    trio = lambda c: pl.BlockSpec((3, PAIR, c), lambda i: (0, i, 0))
    return pl.pallas_call(
        attn_fwd_kernel,
        grid=(pairs,),
        in_specs=[trio(width), trio(1), pl.BlockSpec((width, tokens), lambda i: (0, 0), pipeline_mode=pl.Buffered(1))],
        out_specs=[trio(tokens), pl.BlockSpec((PAIR, tokens), lambda i: (i, 0)),
                   pl.BlockSpec((1, 8, tokens), lambda i: (i, 0, 0))],
        out_shape=[jax.ShapeDtypeStruct((3, rows, tokens), BF16), jax.ShapeDtypeStruct((rows, tokens), BF16),
                   jax.ShapeDtypeStruct((pairs, 8, tokens), F32)],
        cost_estimate=pl.CostEstimate(flops=flops, bytes_accessed=14 * rows * tokens, transcendentals=0),
        name="af",
    )(w, bias, h_one)


def attn_bwd(qkv, d_mixed, lse, h_one):
    _, rows, tokens = qkv.shape
    width = h_one.shape[1]
    pairs = rows // PAIR
    flops = 40 * rows * tokens * tokens + 6 * rows * tokens * width
    trio = lambda c: pl.BlockSpec((3, PAIR, c), lambda i: (0, i, 0))
    return pl.pallas_call(
        attn_bwd_kernel,
        grid=(pairs,),
        in_specs=[trio(tokens), pl.BlockSpec((PAIR, tokens), lambda i: (i, 0)), pl.BlockSpec((1, 8, tokens), lambda i: (i, 0, 0)),
                  pl.BlockSpec((tokens, width), lambda i: (0, 0), pipeline_mode=pl.Buffered(1))],
        out_specs=[trio(tokens), trio(width), pl.BlockSpec((3, 1, 8, PAIR), lambda i: (0, i, 0, 0))],
        out_shape=[jax.ShapeDtypeStruct((3, rows, tokens), BF16), jax.ShapeDtypeStruct((3, rows, width), F32),
                   jax.ShapeDtypeStruct((3, pairs, 8, PAIR), F32)],
        scratch_shapes=[pltpu.VMEM((2, tokens, HEAD), F32), pltpu.VMEM((2, tokens, HEAD), F32)],
        cost_estimate=pl.CostEstimate(flops=flops, bytes_accessed=30 * rows * tokens, transcendentals=0),
        name="ab",
    )(qkv, d_mixed, lse, h_one)


def gelu_and_slope(pre_act):
    square = pre_act * pre_act
    bend = jnp.tanh(GELU_C * pre_act * (1.0 + 0.044715 * square))
    half = 0.5 * (1.0 + bend)
    slope = half + 0.5 * pre_act * (1.0 - bend * bend) * (GELU_C * (1.0 + 3 * 0.044715 * square))
    return pre_act * half, slope


def mlp_in_kernel(h_ref, wa_ref, wb_ref, ba_ref, bb_ref, ua_ref, ub_ref):
    ua_ref[...] = (dot_nt(h_ref[...], wa_ref[...]) + ba_ref[...]).astype(BF16)
    ub_ref[...] = (dot_nt(h_ref[...], wb_ref[...]) + bb_ref[...]).astype(BF16)


def mlp_block(u_ref, d_ref, w1_ref, w2_ref):
    g, slope = gelu_and_slope(u_ref[...].astype(F32))
    g = g.astype(BF16)
    d_g = dot_nt(d_ref[...], w2_ref[...]).astype(BF16).astype(F32)
    d_u = (d_g * slope).astype(BF16)
    return g, d_u, dot(g, w2_ref[...]), dot(d_u, w1_ref[...])


def add_row_sum(sum_ref, rows):
    part = dot(jnp.ones((8, rows.shape[0]), BF16), rows)[:1] if rows.dtype == BF16 else jnp.sum(rows, axis=0, keepdims=True)

    @pl.when(pl.program_id(0) == 0)
    def _():
        sum_ref[...] = part

    @pl.when(pl.program_id(0) > 0)
    def _():
        sum_ref[...] += part


def mlp_near_kernel(ua_ref, ub_ref, d_ref, w1a_ref, w1b_ref, w2a_ref, w2b_ref, g_ref, du_ref, y_ref, dh_ref, dus_ref, ds_ref):
    g, d_u, y, d_h = mlp_block(ua_ref, d_ref, w1a_ref, w2a_ref)
    g_ref[...] = g
    du_ref[...] = d_u
    add_row_sum(dus_ref, d_u)
    add_row_sum(ds_ref, d_ref[...])
    _, _, y_b, d_h_b = mlp_block(ub_ref, d_ref, w1b_ref, w2b_ref)
    y_ref[...] = y + y_b
    dh_ref[...] = d_h + d_h_b


def norm_bwd_tile(x_ref, d_h, res_ref, gain_ref, out_ref, dgain_ref, dbias_ref, dout_ref):
    x = x_ref[...].astype(F32)
    centered = x - jnp.mean(x, axis=-1, keepdims=True)
    inv = lax.rsqrt(jnp.mean(centered * centered, axis=-1, keepdims=True) + LN_EPS)
    unit = centered * inv
    add_row_sum(dbias_ref, d_h)
    d_h = d_h.astype(F32)
    d_unit = d_h * gain_ref[...]
    tilt = jnp.mean(d_unit * unit, axis=-1, keepdims=True)
    d_x = inv * (d_unit - jnp.mean(d_unit, axis=-1, keepdims=True) - unit * tilt)
    out = (res_ref[...].astype(F32) + d_x).astype(BF16)
    out_ref[...] = out
    add_row_sum(dgain_ref, d_h * unit)
    if dout_ref is not None:
        add_row_sum(dout_ref, out)


def norm_one_kernel(*refs):
    d_refs, (x_ref, res_ref), w_refs, rest = refs[:4], refs[4:6], refs[6:10], refs[10:]
    d_h = dot_tn(d_refs[0][...], w_refs[0][...])
    for d_ref, w_ref in zip(d_refs[1:], w_refs[1:]):
        d_h += dot_tn(d_ref[...], w_ref[...])
    gain_ref, out_ref, dgain_ref, dbias_ref = rest
    norm_bwd_tile(x_ref, d_h.astype(BF16), res_ref, gain_ref, out_ref, dgain_ref, dbias_ref, None)


def norm_one_bwd(d_qkv, w_qkv, x, residual, gain):
    tokens, width = x.shape
    tile = 256
    rows = pl.BlockSpec((tile, width), lambda i: (i, 0))
    whole = lambda op: pl.BlockSpec(op.shape, lambda i: (0, 0), pipeline_mode=pl.Buffered(1))
    depth = d_qkv[0].shape[0]
    return pl.pallas_call(
        norm_one_kernel,
        grid=(tokens // tile,),
        in_specs=[pl.BlockSpec((depth, tile), lambda i: (0, i))] * 4 + [rows, rows] + [whole(w) for w in w_qkv] + [whole(gain)],
        out_specs=[rows] + [pl.BlockSpec((1, width), lambda i: (0, 0))] * 2,
        out_shape=[jax.ShapeDtypeStruct((tokens, width), BF16)] + [jax.ShapeDtypeStruct((1, width), F32)] * 2,
        cost_estimate=pl.CostEstimate(flops=8 * depth * tokens * width, bytes_accessed=30 * depth * tokens, transcendentals=0),
        name="nob",
    )(*d_qkv, x, residual, *w_qkv, gain)


def mlp_far_kernel(ua_ref, ub_ref, d_ref, w1a_ref, w1b_ref, w2a_ref, w2b_ref, x_ref, b_ref, gain_ref, yp_ref, dhp_ref,
                   y_ref, out_ref, dgain_ref, dbias_ref, dout_ref):
    _, _, y, d_h = mlp_block(ua_ref, d_ref, w1a_ref, w2a_ref)
    _, _, y_b, d_h_b = mlp_block(ub_ref, d_ref, w1b_ref, w2b_ref)
    y_ref[...] = (x_ref[...].astype(F32) + (yp_ref[...] + (y + y_b)) + b_ref[...]).astype(BF16)
    d_h = (dhp_ref[...] + (d_h + d_h_b)).astype(BF16)
    norm_bwd_tile(x_ref, d_h, d_ref, gain_ref, out_ref, dgain_ref, dbias_ref, dout_ref)


def mlp_own_kernel(h_ref, d_ref, w1_ref, w2_ref, b_ref, g_ref, du_ref, dus_ref):
    u = (dot_nt(h_ref[...], w1_ref[...]) + b_ref[...]).astype(BF16)
    g, slope = gelu_and_slope(u.astype(F32))
    g_ref[...] = g.astype(BF16)
    d_g = dot_nt(d_ref[...], w2_ref[...]).astype(BF16).astype(F32)
    d_u = (d_g * slope).astype(BF16)
    du_ref[...] = d_u
    add_row_sum(dus_ref, d_u)


def row_call(kernel, tiled, fixed, outs, flops, order=None, sums=(), tile=ROWS):
    rows = tiled[0].shape[0]
    operands = tiled + fixed if order is None else [(tiled + fixed)[i] for i in order]
    is_tiled = [True] * len(tiled) + [False] * len(fixed)
    is_tiled = is_tiled if order is None else [is_tiled[i] for i in order]
    in_specs = [pl.BlockSpec((tile, op.shape[1]), lambda i: (i, 0)) if t
                else pl.BlockSpec(op.shape, lambda i: (0, 0), pipeline_mode=pl.Buffered(1))
                for op, t in zip(operands, is_tiled)]
    size = sum(op.size * op.dtype.itemsize for op in operands) + sum(rows * c * d.dtype.itemsize for c, d in
                                                                     [(c, jnp.zeros((), d)) for c, d in outs])
    return pl.pallas_call(
        kernel,
        grid=(rows // tile,),
        in_specs=in_specs,
        out_specs=[pl.BlockSpec((tile, c), lambda i: (i, 0)) for c, _ in outs] + [pl.BlockSpec((1, c), lambda i: (0, 0)) for c in sums],
        out_shape=[jax.ShapeDtypeStruct((rows, c), d) for c, d in outs] + [jax.ShapeDtypeStruct((1, c), F32) for c in sums],
        cost_estimate=pl.CostEstimate(flops=flops, bytes_accessed=size, transcendentals=0),
    )(*operands)


def solution(mesh):
    act_spec = P('dp', 'tp', None)
    replicated = P()
    head_w = P(None, 'tp', None)
    head_b = P('tp', None)
    grad_head_w = P('dp', 'tp', None)
    grad_head_b = P(('dp', 'tp'), None)
    grad_vec = P('dp')
    in_specs = (act_spec, act_spec, replicated, replicated, head_w, head_b, head_w, head_w, head_b,
                P('tp', None, None), replicated, replicated, replicated, P(None, 'tp'), P('tp'), P('tp', None), replicated)
    out_specs = (act_spec, act_spec, grad_vec, grad_vec, grad_head_w, grad_head_b, grad_head_w, grad_head_w, grad_head_b,
                 P(('dp', 'tp'), None, None), grad_vec, grad_vec, grad_vec, P('dp', 'tp'), P(('dp', 'tp')),
                 P(('dp', 'tp'), None), grad_vec)

    def swap(value, k):
        return lax.ppermute(value, 'tp', [(i, i ^ k) for i in range(4)])

    def send(block):
        return block, swap(block, 1), swap(block, 2)

    def land(sent, dep):
        own, near, two = sent
        two, _ = lax.optimization_barrier((two, dep))
        return [own, near, two, swap(two, 1)]

    def layer_step(x, d_out, ln1_gain, ln1_bias, w_q, b_q, w_k, w_v, b_v, w_o, b_o, ln2_gain, ln2_bias, w_1, b_1, w_2, b_2):
        me = lax.axis_index('tp')
        width = x.shape[2]
        slab = x.shape[1]
        local_rows = w_o.shape[0] * w_o.shape[1]

        def image(shard, k):
            return lax.dynamic_index_in_dim(shard, me ^ k, 0, keepdims=False)

        def to_image(shard):
            return jnp.concatenate([image(shard, 0)] + [swap(image(shard, k), k) for k in (1, 2, 3)], axis=0)

        def to_tokens(rows):
            parts = [rows[:slab]] + [swap(rows[k * slab:(k + 1) * slab], k) for k in (1, 2, 3)]
            stacked = jnp.stack(parts)
            return jnp.stack([lax.dynamic_index_in_dim(stacked, me ^ i, 0, keepdims=False) for i in range(4)])

        x_img = to_image(x)
        w_qkv_own = jnp.stack([w.reshape(width, local_rows).T for w in (w_q, w_k, w_v)])
        w_qkv_sent = send(w_qkv_own)
        w_out_sent = send(w_o.reshape(local_rows, width))
        bias_own = jnp.concatenate([b_q.reshape(-1).astype(F32), b_v.reshape(-1).astype(F32), b_1.astype(F32)])
        biases = send(bias_own)
        biases = list(biases) + [swap(biases[2], 1)]
        b_qkv = [jnp.stack([b[:local_rows], jnp.zeros((local_rows,), F32), b[local_rows:2 * local_rows]])[:, :, None]
                 for b in biases]
        b_one = [b[2 * local_rows:] for b in biases]
        w_one_own = w_1.T
        w_one_sent = send(w_one_own)
        core, chip = lax.rem(me, 2), lax.div(me, 2)
        d_here = lax.dynamic_slice_in_dim(d_out, 2 * chip, 2, 0)
        d_there = lax.dynamic_slice_in_dim(d_out, 2 - 2 * chip, 2, 0)
        d_here_near, d_here_two = swap(d_here, 1), swap(d_there, 2)
        w_two_sent = send(w_2)
        d_there_near, d_there_two = swap(d_there, 1), swap(d_here, 2)

        def rows_of(pairs, which):
            return jnp.concatenate([lax.dynamic_index_in_dim(p, which, 0, keepdims=False) for p in pairs], axis=0)

        x_f32 = x_img.astype(F32)
        h_one = layer_norm(x_f32, ln1_gain, ln1_bias).astype(BF16)
        h_one_t = lax.optimization_barrier(h_one.T)
        qkv, mixed, lse = [], [], []
        w_qkv = list(w_qkv_sent[:2])
        for k in range(4):
            if k == 2:
                w_qkv = land(w_qkv_sent, mixed[1])
            block, out, stat = attn_fwd(w_qkv[k], b_qkv[k], h_one_t)
            qkv.append(block)
            mixed.append(out)
            lse.append(stat)
        w_out = land(w_out_sent, mixed[2])
        attn_out = dot_tn(jnp.concatenate(mixed, axis=0), jnp.concatenate(w_out, axis=0))
        x_mid = (x_f32 + attn_out + b_o).astype(BF16)
        mid_f32 = x_mid.astype(F32)
        h_two = layer_norm(mid_f32, ln2_gain, ln2_bias).astype(BF16)
        h_sent = send(h_two)

        cols = w_1.shape[1]
        mm = 2 * h_two.shape[0] * width * cols
        b_one = [b[None, :] for b in b_one]

        def mlp_in(w, b):
            return row_call(mlp_in_kernel, [h_two], [*w, *b], [(cols, BF16)] * 2, 2 * mm)

        pre_near = mlp_in(w_one_sent[:2], b_one[:2])

        def own_columns(h_rows, d_rows):
            g, d_u, d_u_sum = row_call(mlp_own_kernel, [h_rows, d_rows], [w_one_own, w_2, b_one[0]], [(cols, BF16)] * 2,
                                       2 * mm * (h_rows.shape[0] // h_two.shape[0]), sums=(cols,))
            return h_rows, d_rows, g, d_u, d_u_sum

        d_here_two, _ = lax.optimization_barrier((d_here_two, pre_near[1]))
        d_here_diag = swap(d_here_two, 1)
        d_img = rows_of((d_here, d_here_near, d_here_two, d_here_diag), core)
        d_sib = rows_of((d_here_near, d_here, d_here_diag, d_here_two), 1 - core)
        g_own, d_u_own, y_part, d_h_part, d_u_sum, d_sum = row_call(
            mlp_near_kernel, [*pre_near, d_img], [*w_one_sent[:2], *w_two_sent[:2]],
            [(cols, BF16)] * 2 + [(width, F32)] * 2, 6 * mm, sums=(cols, width))
        part_sib = own_columns(h_sent[1], d_sib)
        w_one = land(w_one_sent, (part_sib[3], y_part))
        pre_far = mlp_in(w_one[2:], b_one[2:])
        parts = [(h_two, d_img, g_own, d_u_own, d_u_sum), part_sib]
        g_w_1 = sum(dot_tn(p[3], p[0]) for p in parts)
        g_w_2 = sum(dot_tn(p[2], p[1]) for p in parts)
        g_w_1, g_w_2 = lax.optimization_barrier((g_w_1, g_w_2))
        w_two = land(w_two_sent, pre_far[1])
        y_img, d_mid, g_ln2_gain, g_ln2_bias, d_mid_sum = row_call(
            mlp_far_kernel, [*pre_far, d_img, x_mid, y_part, d_h_part],
            [*w_one[2:], *w_two[2:], b_2.astype(F32)[None, :], ln2_gain[None, :]], [(width, BF16)] * 2, 6 * mm,
            order=(0, 1, 2, 6, 7, 8, 9, 3, 10, 11, 4, 5), sums=(width,) * 3)
        y_out = to_tokens(y_img)

        def reduce_cross(part):
            return swap(part[2] + swap(part[3], 1), 2)

        def reduce_near(part, crossed):
            return part[0] + swap(part[1], 1) + crossed

        g_o_part = [dot(mixed[k], d_mid) for k in range(4)]
        g_w_o = reduce_near(g_o_part, reduce_cross(g_o_part))
        d_qkv, g_qkv_part, b_part = [None] * 4, [None] * 4, [None] * 4
        for k in (3, 2, 1, 0):
            d_mixed = dot_nt(w_out[k], d_mid).astype(BF16)
            d_qkv[k], g_qkv_part[k], b_part[k] = attn_bwd(qkv[k], d_mixed, lse[k], h_one)
        g_w_qkv = reduce_near(g_qkv_part, reduce_cross(g_qkv_part)).astype(BF16)
        g_w_q, g_w_k, g_w_v = [g_w_qkv[i].T.reshape(w_q.shape) for i in range(3)]

        grad_x_img, g_ln1_gain, g_ln1_bias = norm_one_bwd(
            [d.reshape(-1, d.shape[2]) for d in d_qkv], [w.reshape(-1, width) for w in w_qkv], x_img, d_mid, ln1_gain[None, :])
        h_all = land(h_sent, grad_x_img)
        d_there_two, _ = lax.optimization_barrier((d_there_two, d_mid))
        d_there_diag = swap(d_there_two, 1)
        d_far = jnp.concatenate([rows_of((d_there_two, d_there_diag, d_there, d_there_near), core),
                                 rows_of((d_there_diag, d_there_two, d_there_near, d_there), 1 - core)], axis=0)
        part_far = own_columns(jnp.concatenate(h_all[2:], axis=0), d_far)
        g_w_1 = (g_w_1 + dot_tn(part_far[3], part_far[0])).astype(BF16).T
        g_w_2 = (g_w_2 + dot_tn(part_far[2], part_far[1])).astype(BF16)
        g_b_1 = (parts[0][4] + parts[1][4] + part_far[4])[0].astype(BF16)
        grad_x = to_tokens(grad_x_img)

        b_part = [b[:, :, 0] for b in b_part]
        g_b_qkv = reduce_near(b_part, reduce_cross(b_part)).astype(BF16)
        vecs = jnp.concatenate([g_ln1_gain, g_ln1_bias, d_mid_sum, g_ln2_gain, g_ln2_bias, d_sum], axis=0)
        vecs = vecs + swap(vecs, 1)
        vecs = vecs + swap(vecs, 2)
        return (y_out, grad_x, vecs[0], vecs[1], g_w_q, g_b_qkv[0].reshape(b_q.shape), g_w_k, g_w_v,
                g_b_qkv[2].reshape(b_v.shape), g_w_o.astype(BF16).reshape(w_o.shape),
                vecs[2].astype(BF16), vecs[3], vecs[4], g_w_1, g_b_1, g_w_2, vecs[5].astype(BF16))

    return jax.shard_map(layer_step, mesh=mesh, in_specs=in_specs, out_specs=out_specs, check_vma=False)
```

```python
import math
import jax
import jax.numpy as jnp
from jax import lax
from jax.experimental import pallas as pl
from jax.experimental.pallas import tpu as pltpu
from jax.sharding import PartitionSpec as P

LN_EPS = 1e-6
HEAD = 72
PAIR = 2 * HEAD
FWD_QUERIES = 1024
BWD_QUERIES = 512
ROWS = 256
GELU_C = math.sqrt(2.0 / math.pi)
F32 = jnp.float32
BF16 = jnp.bfloat16
LOG2E = 1.4426950408889634


def by_row(i, *_):
    return i, 0


def stay(*_):
    return 0, 0


def layer_norm(rows, ln_gain, ln_bias):
    row_mean = jnp.mean(rows, axis=-1, keepdims=True)
    centered = rows - row_mean
    variance = jnp.mean(centered * centered, axis=-1, keepdims=True)
    return centered * lax.rsqrt(variance + LN_EPS) * ln_gain + ln_bias


def dot(a, b):
    return jnp.dot(a, b, preferred_element_type=F32)


def dot_nt(a, b):
    return lax.dot_general(a, b, (((1,), (1,)), ((), ())), preferred_element_type=F32)


def dot_tn(a, b):
    return lax.dot_general(a, b, (((0,), (0,)), ((), ())), preferred_element_type=F32)


def attn_fwd_kernel(w_ref, b_ref, h_ref, qkv_ref, o_ref, l_ref):
    tokens = h_ref.shape[1]
    coef = LOG2E / math.sqrt(HEAD)
    parts = [(dot(w_ref[i], h_ref[...]) + b_ref[i]).astype(BF16) for i in range(3)]
    for i in range(3):
        qkv_ref[i] = parts[i]
    q_all, k_all, v_all = [part.astype(F32) for part in parts]
    keys = [k_all[h * HEAD:(h + 1) * HEAD].T.astype(BF16) for h in range(2)]
    vals = [v_all[h * HEAD:(h + 1) * HEAD].astype(BF16) for h in range(2)]
    quer = [q_all[h * HEAD:(h + 1) * HEAD].astype(BF16) for h in range(2)]
    for start in range(0, tokens, FWD_QUERIES):
        outs = []
        for h in range(2):
            s = dot(keys[h], quer[h][:, start:start + FWD_QUERIES])
            top = jnp.max(s, axis=0, keepdims=True)
            e = jnp.exp2((s - top) * coef)
            total = jnp.sum(e, axis=0, keepdims=True)
            p = (e * (1.0 / total)).astype(BF16)
            outs.append(dot(vals[h], p))
            l_ref[0, h:h + 1, start:start + FWD_QUERIES] = top * coef + jnp.log2(total)
        o_ref[:, start:start + FWD_QUERIES] = jnp.concatenate(outs, axis=0).astype(BF16)


def attn_bwd_kernel(qkv_ref, g_ref, l_ref, h_ref, d_ref, gw_ref, gb_ref, dk_acc, dv_acc):
    tokens = h_ref.shape[0]
    scale = 1.0 / math.sqrt(HEAD)
    coef = LOG2E * scale
    q_all, k_all, v_all = [qkv_ref[i].astype(F32) for i in range(3)]
    g_all = g_ref[...].astype(F32)

    def head(a, h):
        return a[h * HEAD:(h + 1) * HEAD]

    k_t = [head(k_all, h).astype(BF16) for h in range(2)]
    keys = [head(k_all, h).T.astype(BF16) for h in range(2)]
    vals = [head(v_all, h).T.astype(BF16) for h in range(2)]
    q_t = [head(q_all, h).astype(BF16) for h in range(2)]
    q_n = [head(q_all, h).T.astype(BF16) for h in range(2)]
    g_t = [head(g_all, h).astype(BF16) for h in range(2)]
    g_n = [head(g_all, h).T.astype(BF16) for h in range(2)]
    for start in range(0, tokens, BWD_QUERIES):
        cols = slice(start, start + BWD_QUERIES)
        dqs = []
        for h in range(2):
            s = dot(keys[h], q_t[h][:, cols])
            p = jnp.exp2(s * coef - l_ref[0, h:h + 1, cols])
            dp = dot(vals[h], g_t[h][:, cols]).astype(BF16).astype(F32)
            delta = jnp.sum(p * dp, axis=0, keepdims=True)
            ds = (p * ((dp - delta) * scale)).astype(BF16)
            dv = dot(p.astype(BF16), g_n[h][cols])
            dk = dot(ds, q_n[h][cols])
            if start == 0:
                dv_acc[h] = dv
                dk_acc[h] = dk
            else:
                dv_acc[h] += dv
                dk_acc[h] += dk
            dqs.append(dot(k_t[h], ds))
        d_ref[0, :, cols] = jnp.concatenate(dqs, axis=0).astype(BF16)
    d_ref[1] = jnp.concatenate([dk_acc[h].T for h in range(2)], axis=0).astype(BF16)
    d_ref[2] = jnp.concatenate([dv_acc[h].T for h in range(2)], axis=0).astype(BF16)
    ones = jnp.ones((8, tokens), BF16)
    for i in range(3):
        gw_ref[i] = dot(d_ref[i], h_ref[...])
        gb_ref[i, 0] = dot_nt(ones, d_ref[i])


def attn_fwd(w, bias, h_one):
    _, rows, width = w.shape
    tokens = h_one.shape[1]
    pairs = rows // PAIR
    flops = 16 * rows * tokens * tokens + 6 * rows * tokens * width
    trio = lambda c: pl.BlockSpec((3, PAIR, c), lambda i: (0, i, 0))
    return pl.pallas_call(
        attn_fwd_kernel,
        grid=(pairs,),
        in_specs=[trio(width), trio(1), pl.BlockSpec((width, tokens), stay, pipeline_mode=pl.Buffered(1))],
        out_specs=[trio(tokens), pl.BlockSpec((PAIR, tokens), by_row),
                   pl.BlockSpec((1, 8, tokens), lambda i: (i, 0, 0))],
        out_shape=[jax.ShapeDtypeStruct((3, rows, tokens), BF16), jax.ShapeDtypeStruct((rows, tokens), BF16),
                   jax.ShapeDtypeStruct((pairs, 8, tokens), F32)],
        cost_estimate=pl.CostEstimate(flops=flops, bytes_accessed=14 * rows * tokens, transcendentals=0),
        name="af",
    )(w, bias, h_one)


def attn_bwd(qkv, d_mixed, lse, h_one):
    _, rows, tokens = qkv.shape
    width = h_one.shape[1]
    pairs = rows // PAIR
    flops = 40 * rows * tokens * tokens + 6 * rows * tokens * width
    trio = lambda c: pl.BlockSpec((3, PAIR, c), lambda i: (0, i, 0))
    return pl.pallas_call(
        attn_bwd_kernel,
        grid=(pairs,),
        in_specs=[trio(tokens), pl.BlockSpec((PAIR, tokens), by_row), pl.BlockSpec((1, 8, tokens), lambda i: (i, 0, 0)),
                  pl.BlockSpec((tokens, width), stay, pipeline_mode=pl.Buffered(1))],
        out_specs=[trio(tokens), trio(width), pl.BlockSpec((3, 1, 8, PAIR), lambda i: (0, i, 0, 0))],
        out_shape=[jax.ShapeDtypeStruct((3, rows, tokens), BF16), jax.ShapeDtypeStruct((3, rows, width), F32),
                   jax.ShapeDtypeStruct((3, pairs, 8, PAIR), F32)],
        scratch_shapes=[pltpu.VMEM((2, tokens, HEAD), F32), pltpu.VMEM((2, tokens, HEAD), F32)],
        cost_estimate=pl.CostEstimate(flops=flops, bytes_accessed=30 * rows * tokens, transcendentals=0),
        name="ab",
    )(qkv, d_mixed, lse, h_one)


def gelu_and_slope(pre_act):
    square = pre_act * pre_act
    bend = jnp.tanh(GELU_C * pre_act * (1.0 + 0.044715 * square))
    half = 0.5 * (1.0 + bend)
    slope = half + 0.5 * pre_act * (1.0 - bend * bend) * (GELU_C * (1.0 + 3 * 0.044715 * square))
    return pre_act * half, slope


def mlp_in_kernel(h_ref, wa_ref, wb_ref, ba_ref, bb_ref, ua_ref, ub_ref):
    ua_ref[...] = (dot_nt(h_ref[...], wa_ref[...]) + ba_ref[...]).astype(BF16)
    ub_ref[...] = (dot_nt(h_ref[...], wb_ref[...]) + bb_ref[...]).astype(BF16)


def mlp_block(u_ref, d_ref, w1_ref, w2_ref):
    g, slope = gelu_and_slope(u_ref[...].astype(F32))
    g = g.astype(BF16)
    d_g = dot_nt(d_ref[...], w2_ref[...]).astype(BF16).astype(F32)
    d_u = (d_g * slope).astype(BF16)
    return g, d_u, dot(g, w2_ref[...]), dot(d_u, w1_ref[...])


def add_row_sum(sum_ref, rows):
    part = dot(jnp.ones((8, rows.shape[0]), BF16), rows)[:1] if rows.dtype == BF16 else jnp.sum(rows, axis=0, keepdims=True)

    @pl.when(pl.program_id(0) == 0)
    def _():
        sum_ref[...] = part

    @pl.when(pl.program_id(0) > 0)
    def _():
        sum_ref[...] += part


def mlp_near_kernel(ua_ref, ub_ref, d_ref, w1a_ref, w1b_ref, w2a_ref, w2b_ref, g_ref, du_ref, y_ref, dh_ref, dus_ref, ds_ref):
    g, d_u, y, d_h = mlp_block(ua_ref, d_ref, w1a_ref, w2a_ref)
    g_ref[...] = g
    du_ref[...] = d_u
    add_row_sum(dus_ref, d_u)
    add_row_sum(ds_ref, d_ref[...])
    _, _, y_b, d_h_b = mlp_block(ub_ref, d_ref, w1b_ref, w2b_ref)
    y_ref[...] = y + y_b
    dh_ref[...] = d_h + d_h_b


def norm_bwd_tile(x_ref, d_h, res_ref, gain_ref, out_refs, dgain_ref, dbias_ref, dout_ref):
    x = x_ref[...].astype(F32)
    centered = x - jnp.mean(x, axis=-1, keepdims=True)
    inv = lax.rsqrt(jnp.mean(centered * centered, axis=-1, keepdims=True) + LN_EPS)
    unit = centered * inv
    add_row_sum(dbias_ref, d_h)
    d_h = d_h.astype(F32)
    d_unit = d_h * gain_ref[...]
    tilt = jnp.mean(d_unit * unit, axis=-1, keepdims=True)
    d_x = inv * (d_unit - jnp.mean(d_unit, axis=-1, keepdims=True) - unit * tilt)
    out = (res_ref[...].astype(F32) + d_x).astype(BF16)
    store_slab(out_refs, out)
    add_row_sum(dgain_ref, d_h * unit)
    if dout_ref is not None:
        add_row_sum(dout_ref, out)


def store_slab(refs, rows):
    if len(refs) == 1:
        refs[0][...] = rows
        return
    for k, ref in enumerate(refs):
        @pl.when(pl.program_id(0) == k)
        def _(ref=ref):
            ref[...] = rows


def norm_one_kernel(*refs):
    d_refs, (x_ref, res_ref), w_refs, rest = refs[:4], refs[4:6], refs[6:10], refs[10:]
    d_h = dot_tn(d_refs[0][...], w_refs[0][...])
    for d_ref, w_ref in zip(d_refs[1:], w_refs[1:]):
        d_h += dot_tn(d_ref[...], w_ref[...])
    gain_ref, outs, (dgain_ref, dbias_ref) = rest[0], rest[1:5], rest[5:]
    norm_bwd_tile(x_ref, d_h.astype(BF16), res_ref, gain_ref, outs, dgain_ref, dbias_ref, None)


def norm_one_bwd(d_qkv, w_qkv, x, residual, gain):
    tokens, width = x.shape
    tile = tokens // 4
    rows = pl.BlockSpec((tile, width), by_row)
    whole = lambda op: pl.BlockSpec(op.shape, stay, pipeline_mode=pl.Buffered(1))
    depth = d_qkv[0].shape[0]
    return pl.pallas_call(
        norm_one_kernel,
        grid=(tokens // tile,),
        in_specs=[pl.BlockSpec((depth, tile), lambda i: (0, i))] * 4 + [rows, rows] + [whole(w) for w in w_qkv] + [whole(gain)],
        out_specs=[pl.BlockSpec((tile, width), stay)] * 4 + [pl.BlockSpec((1, width), stay)] * 2,
        out_shape=[jax.ShapeDtypeStruct((tile, width), BF16)] * 4 + [jax.ShapeDtypeStruct((1, width), F32)] * 2,
        cost_estimate=pl.CostEstimate(flops=8 * depth * tokens * width, bytes_accessed=30 * depth * tokens, transcendentals=0),
        name="nob",
    )(*d_qkv, x, residual, *w_qkv, gain)


def mlp_far_kernel(ua_ref, ub_ref, d_ref, w1a_ref, w1b_ref, w2a_ref, w2b_ref, x_ref, b_ref, gain_ref, yp_ref, dhp_ref,
                   out_ref, dgain_ref, dbias_ref, dout_ref, *y_refs):
    _, _, y, d_h = mlp_block(ua_ref, d_ref, w1a_ref, w2a_ref)
    _, _, y_b, d_h_b = mlp_block(ub_ref, d_ref, w1b_ref, w2b_ref)
    store_slab(y_refs, (x_ref[...].astype(F32) + (yp_ref[...] + (y + y_b)) + b_ref[...]).astype(BF16))
    d_h = (dhp_ref[...] + (d_h + d_h_b)).astype(BF16)
    norm_bwd_tile(x_ref, d_h, d_ref, gain_ref, (out_ref,), dgain_ref, dbias_ref, dout_ref)


def mlp_own_kernel(h_ref, d_ref, w1_ref, w2_ref, b_ref, g_ref, du_ref, dus_ref):
    u = (dot_nt(h_ref[...], w1_ref[...]) + b_ref[...]).astype(BF16)
    g, slope = gelu_and_slope(u.astype(F32))
    g_ref[...] = g.astype(BF16)
    d_g = dot_nt(d_ref[...], w2_ref[...]).astype(BF16).astype(F32)
    d_u = (d_g * slope).astype(BF16)
    du_ref[...] = d_u
    add_row_sum(dus_ref, d_u)


def gather_rows_kernel(core_ref, a_ref, b_ref, c_ref, d_ref, out_ref):
    refs = (a_ref, b_ref, c_ref, d_ref)
    for step in range(8):
        @pl.when(pl.program_id(0) == step)
        def _(step=step):
            out_ref[...] = refs[(step % 4) ^ (step // 4)][0]


def gather_rows(core, slabs, images=2):
    _, tokens, width = slabs[0].shape
    pick = lambda i, core: (lax.rem(core[0] + lax.div(i, 4), 2), 0, 0)
    return pl.pallas_call(
        gather_rows_kernel,
        grid_spec=pltpu.PrefetchScalarGridSpec(
            num_scalar_prefetch=1, grid=(4 * images,),
            in_specs=[pl.BlockSpec((1, tokens, width), pick)] * 4,
            out_specs=pl.BlockSpec((tokens, width), by_row)),
        out_shape=jax.ShapeDtypeStruct((4 * images * tokens, width), slabs[0].dtype),
        cost_estimate=pl.CostEstimate(flops=30 * 8 * tokens * width, bytes_accessed=32 * tokens * width, transcendentals=0),
        name="gr",
    )(core[None], *slabs)


def mlp_own_far_kernel(core_ref, ha_ref, hb_ref, da_ref, db_ref, dc_ref, dd_ref, w1_ref, w2_ref, b_ref,
                       g_ref, du_ref, h_ref, d_ref, dus_ref):
    gather_rows_kernel(core_ref, da_ref, db_ref, dc_ref, dd_ref, d_ref)

    @pl.when(pl.program_id(0) < 4)
    def _():
        h_ref[...] = ha_ref[...]

    @pl.when(pl.program_id(0) >= 4)
    def _():
        h_ref[...] = hb_ref[...]

    mlp_own_kernel(h_ref, d_ref, w1_ref, w2_ref, b_ref, g_ref, du_ref, dus_ref)


def mlp_own_far(core, h_two, h_diag, slabs, w_1, w_2, b_1):
    _, tokens, width = slabs[0].shape
    cols = w_1.shape[0]
    pick = lambda i, core: (lax.rem(core[0] + lax.div(i, 4), 2), 0, 0)
    fixed = lambda op: pl.BlockSpec(op.shape, stay, pipeline_mode=pl.Buffered(1))
    tile = lambda c: pl.BlockSpec((tokens, c), by_row)
    return pl.pallas_call(
        mlp_own_far_kernel,
        grid_spec=pltpu.PrefetchScalarGridSpec(
            num_scalar_prefetch=1, grid=(8,),
            in_specs=[pl.BlockSpec((tokens, width), lambda i, core: (jnp.minimum(i, 3), 0)),
                      pl.BlockSpec((tokens, width), lambda i, core: (jnp.maximum(i - 4, 0), 0))]
            + [pl.BlockSpec((1, tokens, width), pick)] * 4 + [fixed(w_1), fixed(w_2), fixed(b_1)],
            out_specs=[tile(cols), tile(cols), tile(width), tile(width), pl.BlockSpec((1, cols), stay)]),
        out_shape=[jax.ShapeDtypeStruct((8 * tokens, c), BF16) for c in (cols, cols, width, width)]
        + [jax.ShapeDtypeStruct((1, cols), F32)],
        cost_estimate=pl.CostEstimate(flops=32 * tokens * width * cols, bytes_accessed=64 * tokens * width, transcendentals=0),
        name="mof",
    )(core[None], h_two, h_diag, *slabs, w_1, w_2, b_1)


def order_kernel(me_ref, a_ref, b_ref, c_ref, d_ref, out_ref):
    refs = (a_ref, b_ref, c_ref, d_ref)
    for step in range(4):
        @pl.when(pl.program_id(0) == step)
        def _(step=step):
            out_ref[0] = refs[step][...]


def order_parts(me, parts):
    tokens, width = parts[0].shape
    return pl.pallas_call(
        order_kernel,
        grid_spec=pltpu.PrefetchScalarGridSpec(
            num_scalar_prefetch=1, grid=(4,),
            in_specs=[pl.BlockSpec((tokens, width), stay)] * 4,
            out_specs=pl.BlockSpec((1, tokens, width), lambda i, me: (me[0] ^ i, 0, 0))),
        out_shape=jax.ShapeDtypeStruct((4, tokens, width), parts[0].dtype),
        cost_estimate=pl.CostEstimate(flops=30 * 4 * tokens * width, bytes_accessed=16 * tokens * width, transcendentals=0),
        name="op",
    )(me[None], *parts)


def row_call(kernel, tiled, fixed, outs, flops, order=None, sums=(), slabs=0):
    tile = ROWS
    rows = tiled[0].shape[0]
    operands = tiled + fixed if order is None else [(tiled + fixed)[i] for i in order]
    is_tiled = [True] * len(tiled) + [False] * len(fixed)
    is_tiled = is_tiled if order is None else [is_tiled[i] for i in order]
    in_specs = [pl.BlockSpec((tile, op.shape[1]), by_row) if t
                else pl.BlockSpec(op.shape, stay, pipeline_mode=pl.Buffered(1))
                for op, t in zip(operands, is_tiled)]
    size = sum(op.size * op.dtype.itemsize for op in operands) + sum(rows * c * d.dtype.itemsize for c, d in
                                                                     [(c, jnp.zeros((), d)) for c, d in outs])
    return pl.pallas_call(
        kernel,
        grid=(rows // tile,),
        in_specs=in_specs,
        out_specs=[pl.BlockSpec((tile, c), by_row) for c, _ in outs] + [pl.BlockSpec((1, c), stay) for c in sums]
        + [pl.BlockSpec((tile, slabs), stay)] * (4 if slabs else 0),
        out_shape=[jax.ShapeDtypeStruct((rows, c), d) for c, d in outs] + [jax.ShapeDtypeStruct((1, c), F32) for c in sums]
        + [jax.ShapeDtypeStruct((tile, slabs), BF16)] * (4 if slabs else 0),
        cost_estimate=pl.CostEstimate(flops=flops, bytes_accessed=size, transcendentals=0),
    )(*operands)


def solution(mesh):
    act_spec = P('dp', 'tp', None)
    replicated = P()
    head_w = P(None, 'tp', None)
    head_b = P('tp', None)
    grad_head_w = P('dp', 'tp', None)
    grad_head_b = P(('dp', 'tp'), None)
    grad_vec = P('dp')
    in_specs = (act_spec, act_spec, replicated, replicated, head_w, head_b, head_w, head_w, head_b,
                P('tp', None, None), replicated, replicated, replicated, P(None, 'tp'), P('tp'), P('tp', None), replicated)
    out_specs = (act_spec, act_spec, grad_vec, grad_vec, grad_head_w, grad_head_b, grad_head_w, grad_head_w, grad_head_b,
                 P(('dp', 'tp'), None, None), grad_vec, grad_vec, grad_vec, P('dp', 'tp'), P(('dp', 'tp')),
                 P(('dp', 'tp'), None), grad_vec)

    def swap(value, k):
        return lax.ppermute(value, 'tp', [(i, i ^ k) for i in range(4)])

    def send(block):
        return block, swap(block, 1), swap(block, 2)

    def land(sent, dep):
        own, near, two = sent
        two, _ = lax.optimization_barrier((two, dep))
        return [own, near, two, swap(two, 1)]

    def layer_step(x, d_out, ln1_gain, ln1_bias, w_q, b_q, w_k, w_v, b_v, w_o, b_o, ln2_gain, ln2_bias, w_1, b_1, w_2, b_2):
        me = lax.axis_index('tp')
        width = x.shape[2]
        local_rows = w_o.shape[0] * w_o.shape[1]

        def image(shard, k):
            return lax.dynamic_index_in_dim(shard, me ^ k, 0, keepdims=False)

        def to_image(shard):
            return jnp.concatenate([image(shard, 0)] + [swap(image(shard, k), k) for k in (1, 2, 3)], axis=0)

        def to_tokens(slabs):
            parts = [slabs[0]] + [swap(slabs[k], k) for k in (1, 2, 3)]
            return order_parts(me, parts)

        x_img = to_image(x)
        w_qkv_own = jnp.stack([w.reshape(width, local_rows).T for w in (w_q, w_k, w_v)])
        w_qkv_sent = send(w_qkv_own)
        w_out_sent = send(w_o.reshape(local_rows, width))
        bias_own = jnp.concatenate([b_q.reshape(-1).astype(F32), b_v.reshape(-1).astype(F32), b_1.astype(F32)])
        biases = send(bias_own)
        biases = list(biases) + [swap(biases[2], 1)]
        b_qkv = [jnp.stack([b[:local_rows], jnp.zeros((local_rows,), F32), b[local_rows:2 * local_rows]])[:, :, None]
                 for b in biases]
        b_one = [b[2 * local_rows:] for b in biases]
        w_one_own = w_1.T
        w_one_sent = send(w_one_own)
        core, chip = lax.rem(me, 2), lax.div(me, 2)
        d_here = lax.dynamic_slice_in_dim(d_out, 2 * chip, 2, 0)
        d_there = lax.dynamic_slice_in_dim(d_out, 2 - 2 * chip, 2, 0)
        d_here_near, d_here_two = swap(d_here, 1), swap(d_there, 2)
        w_two_sent = send(w_2)
        d_there_near, d_there_two = swap(d_there, 1), swap(d_here, 2)

        x_f32 = x_img.astype(F32)
        h_one = layer_norm(x_f32, ln1_gain, ln1_bias).astype(BF16)
        h_one_t = lax.optimization_barrier(h_one.T)
        qkv, mixed, lse = [], [], []
        w_qkv = list(w_qkv_sent[:2])
        for k in range(4):
            if k == 2:
                w_qkv = land(w_qkv_sent, mixed[1])
            block, out, stat = attn_fwd(w_qkv[k], b_qkv[k], h_one_t)
            qkv.append(block)
            mixed.append(out)
            lse.append(stat)
        w_out = land(w_out_sent, mixed[2])
        attn_out = dot_tn(jnp.concatenate(mixed, axis=0), jnp.concatenate(w_out, axis=0))
        x_mid = (x_f32 + attn_out + b_o).astype(BF16)
        mid_f32 = x_mid.astype(F32)
        h_two = lax.optimization_barrier(layer_norm(mid_f32, ln2_gain, ln2_bias).astype(BF16))
        h_sent = send(h_two)

        cols = w_1.shape[1]
        mm = 2 * h_two.shape[0] * width * cols
        b_one = [b[None, :] for b in b_one]

        def mlp_in(w, b):
            return row_call(mlp_in_kernel, [h_two], [*w, *b], [(cols, BF16)] * 2, 2 * mm)

        pre_near = mlp_in(w_one_sent[:2], b_one[:2])

        def own_columns(h_rows, d_rows):
            g, d_u, d_u_sum = row_call(mlp_own_kernel, [h_rows, d_rows], [w_one_own, w_2, b_one[0]], [(cols, BF16)] * 2,
                                       2 * mm * (h_rows.shape[0] // h_two.shape[0]), sums=(cols,))
            return h_rows, d_rows, g, d_u, d_u_sum

        d_here_two, _ = lax.optimization_barrier((d_here_two, pre_near[1]))
        d_here_diag = swap(d_here_two, 1)
        d_img = gather_rows(core, (d_here, d_here_near, d_here_two, d_here_diag), 1)
        d_sib = gather_rows(1 - core, (d_here_near, d_here, d_here_diag, d_here_two), 1)
        g_own, d_u_own, y_part, d_h_part, d_u_sum, d_sum = row_call(
            mlp_near_kernel, [*pre_near, d_img], [*w_one_sent[:2], *w_two_sent[:2]],
            [(cols, BF16)] * 2 + [(width, F32)] * 2, 6 * mm, sums=(cols, width))
        part_sib = own_columns(h_sent[1], d_sib)
        w_one = land(w_one_sent, (part_sib[3], y_part))
        pre_far = mlp_in(w_one[2:], b_one[2:])
        parts = [(h_two, d_img, g_own, d_u_own, d_u_sum), part_sib]
        g_w_1 = sum(dot_tn(p[3], p[0]) for p in parts)
        g_w_2 = sum(dot_tn(p[2], p[1]) for p in parts)
        g_w_1, g_w_2 = lax.optimization_barrier((g_w_1, g_w_2))
        w_two = land(w_two_sent, pre_far[1])
        d_mid, g_ln2_gain, g_ln2_bias, d_mid_sum, *y_slabs = row_call(
            mlp_far_kernel, [*pre_far, d_img, x_mid, y_part, d_h_part],
            [*w_one[2:], *w_two[2:], b_2.astype(F32)[None, :], ln2_gain[None, :]], [(width, BF16)], 6 * mm,
            order=(0, 1, 2, 6, 7, 8, 9, 3, 10, 11, 4, 5), sums=(width,) * 3, slabs=width)
        y_out = to_tokens(y_slabs)

        def reduce_cross(part):
            return swap(part[2] + swap(part[3], 1), 2)

        def reduce_near(part, crossed):
            return part[0] + swap(part[1], 1) + crossed

        g_o_part = [dot(mixed[k], d_mid) for k in range(4)]
        g_w_o = reduce_near(g_o_part, reduce_cross(g_o_part))
        d_qkv, g_qkv_part, b_part = [None] * 4, [None] * 4, [None] * 4
        for k in (3, 2, 1, 0):
            d_mixed = dot_nt(w_out[k], d_mid).astype(BF16)
            d_qkv[k], g_qkv_part[k], b_part[k] = attn_bwd(qkv[k], d_mixed, lse[k], h_one)
        g_w_qkv = reduce_near(g_qkv_part, reduce_cross(g_qkv_part)).astype(BF16)
        g_w_q, g_w_k, g_w_v = [g_w_qkv[i].T.reshape(w_q.shape) for i in range(3)]

        *grad_x_slabs, g_ln1_gain, g_ln1_bias = norm_one_bwd(
            [d.reshape(-1, d.shape[2]) for d in d_qkv], [w.reshape(-1, width) for w in w_qkv], x_img, d_mid, ln1_gain[None, :])
        h_all = land(h_sent, grad_x_slabs[3])
        d_there_two, _ = lax.optimization_barrier((d_there_two, d_mid))
        d_there_diag = swap(d_there_two, 1)
        g_far, d_u_far, h_far, d_far, d_u_far_sum = mlp_own_far(
            core, h_all[2], h_all[3], (d_there_two, d_there_diag, d_there, d_there_near), w_one_own, w_2, b_one[0])
        g_w_1 = (g_w_1 + dot_tn(d_u_far, h_far)).astype(BF16).T
        g_w_2 = (g_w_2 + dot_tn(g_far, d_far)).astype(BF16)
        g_b_1 = (parts[0][4] + parts[1][4] + d_u_far_sum)[0].astype(BF16)
        grad_x = to_tokens(grad_x_slabs)

        b_part = [b[:, :, 0] for b in b_part]
        g_b_qkv = reduce_near(b_part, reduce_cross(b_part)).astype(BF16)
        vecs = jnp.concatenate([g_ln1_gain, g_ln1_bias, d_mid_sum, g_ln2_gain, g_ln2_bias, d_sum], axis=0)
        vecs = vecs + swap(vecs, 1)
        vecs = vecs + swap(vecs, 2)
        return (y_out, grad_x, vecs[0], vecs[1], g_w_q, g_b_qkv[0].reshape(b_q.shape), g_w_k, g_w_v,
                g_b_qkv[2].reshape(b_v.shape), g_w_o.astype(BF16).reshape(w_o.shape),
                vecs[2].astype(BF16), vecs[3], vecs[4], g_w_1, g_b_1, g_w_2, vecs[5].astype(BF16))

    return jax.shard_map(layer_step, mesh=mesh, in_specs=in_specs, out_specs=out_specs, check_vma=False)
```
